8 devices in a mesh: rep: 1 (over z), r: 2 (over y), s: 4 (over x, core).
Axes of the slice: x: 2, y: 2, z: 1, core: 2. Of those that a mesh axis runs over, the one named last changes fastest.
Arguments:
- x: bfloat16 [8, 4096, 896], P(('rep', 'r', 's'))
- dy: bfloat16 [8, 4096, 896], P(('rep', 'r', 's'))
- w_gate: bfloat16 [2, 896, 2560], P(None, 's')
- w_up: bfloat16 [2, 896, 2560], P(None, 's')
- w_down: bfloat16 [2, 2560, 896], P(None, 's')
- m_w_gate: float32 [2, 896, 2560], P(None, 's')
- m_w_up: float32 [2, 896, 2560], P(None, 's')
- m_w_down: float32 [2, 2560, 896], P(None, 's')
- v_w_gate: float32 [2, 896, 2560], P(None, 's')
- v_w_up: float32 [2, 896, 2560], P(None, 's')
- v_w_down: float32 [2, 2560, 896], P(None, 's')
Outputs:
- output 1: bfloat16 [2, 896, 2560], P('rep', 's')
- output 2: bfloat16 [2, 896, 2560], P('rep', 's')
- output 3: bfloat16 [2, 2560, 896], P('rep', 's')
- output 4: float32 [2, 896, 2560], P('rep', 's')
- output 5: float32 [2, 896, 2560], P('rep', 's')
- output 6: float32 [2, 2560, 896], P('rep', 's')
- output 7: float32 [2, 896, 2560], P('rep', 's')
- output 8: float32 [2, 896, 2560], P('rep', 's')
- output 9: float32 [2, 2560, 896], P('rep', 's')
All inputs are finite; a program needn't handle non-finite values.
Results may differ from the reference program's by a relative error of at most 0.022.
Values are sent between devices in bfloat16 or wider.
A program may use at most 2 GiB of HBM per device.

```python
import jax
import jax.numpy as jnp
from jax import lax

SEQUENCES = 8
TOKENS = 4096
D = 896
FF = 2560
LAYERS = 2
NAMES = ("w_gate", "w_up", "w_down")
SHAPES = {"w_gate": (LAYERS, D, FF), "w_up": (LAYERS, D, FF), "w_down": (LAYERS, FF, D)}


def bump(key, n, height):
    away = (jnp.arange(n, dtype=jnp.int32) - jax.random.randint(key, (), 0, n, jnp.int32)) % n
    return jnp.where(away < n // 8, height, 1.0)


def together(key, own, strength):
    shared = jax.random.normal(key, own.shape[1:], jnp.float32)
    return (own + strength * shared) * lax.rsqrt(1 + strength * strength)


def setup_inputs(seed: int = 0, part: int = 0) -> dict:
    kx, kdy, ka, kb, kz, kf, kh, kl, *keys = jax.random.split(jax.random.key(seed), 8 + 3 * len(NAMES))
    kx, kdy, ka, kb = (jax.random.fold_in(k, part) for k in (kx, kdy, ka, kb))
    kw, km, kv = (keys[i::3] for i in range(3))
    shape = (SEQUENCES, TOKENS, D)
    much_x, much_dy = jax.random.uniform(kz, (2,), jnp.float32, 0.0, 1.0)
    loud = 2.0 ** jax.random.uniform(jax.random.fold_in(kz, 1), (), jnp.float32, -1.0, 2.0)
    layers = 2.0 ** jax.random.uniform(kl, (LAYERS, 1, 1), jnp.float32, -1.0, 1.0)
    x = together(ka, jax.random.normal(kx, shape, jnp.float32), much_x) * bump(kf, D, 4.0)
    dy = together(kb, jax.random.normal(kdy, shape, jnp.float32), much_dy)
    drawn = {"x": x.astype(jnp.bfloat16), "dy": (loud * dy * (SEQUENCES * TOKENS) ** -0.5).astype(jnp.bfloat16)}
    for key, name in zip(kw, NAMES, strict=True):
        w = jax.random.normal(key, SHAPES[name], jnp.float32) * SHAPES[name][1] ** -0.5
        drawn[name] = (w * {"w_gate": 1.0, "w_up": bump(kh, FF, 4.0), "w_down": layers}[name]).astype(jnp.bfloat16)
    for key, name in zip(km, NAMES, strict=True):
        drawn[f"m_{name}"] = 0.1 * jax.random.normal(key, SHAPES[name], jnp.float32)
    for key, name in zip(kv, NAMES, strict=True):
        drawn[f"v_{name}"] = jax.random.uniform(key, SHAPES[name], jnp.float32, 0.005, 0.015)
    return drawn


def matmul(a, w):
    return jnp.dot(a, w, preferred_element_type=jnp.float32).astype(jnp.bfloat16)


def normed(h):
    wide = h.astype(jnp.float32)
    scale = lax.rsqrt(jnp.mean(wide**2, -1, keepdims=True) + 1e-6)
    return (wide * scale).astype(jnp.bfloat16)


def layer(h, w):
    a = normed(h)
    gate = jnp.dot(a, w["w_gate"], preferred_element_type=jnp.float32)
    up = jnp.dot(a, w["w_up"], preferred_element_type=jnp.float32)
    return h + matmul((jax.nn.silu(gate) * up).astype(jnp.bfloat16), w["w_down"])


def adamw(w, m, v, g):
    m = 0.9 * m + 0.1 * g
    v = 0.95 * v + 0.05 * g * g
    step = m * lax.rsqrt(v + 1e-8) + 0.1 * w
    return (w - 0.02 * step).astype(jnp.bfloat16), m, v


def clipped(gradients, sum_of_squares, count):
    factor = jnp.minimum(1.0, 0.5 * lax.rsqrt(sum_of_squares / count + 1e-30))
    return [g * factor for g in gradients]


def stack(weights, h):
    return lax.scan(lambda h, w: (layer(h, w), None), h, weights)[0]


def reference(x, dy, w_gate, w_up, w_down, m_w_gate, m_w_up, m_w_down, v_w_gate, v_w_up, v_w_down):
    weights = dict(zip(NAMES, (w_gate, w_up, w_down), strict=True))

    def take(so_far, sequence):
        h, by_y = sequence
        _, back = jax.vjp(lambda w: stack(w, h), weights)
        return jax.tree.map(lambda total, term: total + term.astype(jnp.float32), so_far, back(by_y)[0]), None

    none_yet = {name: jnp.zeros(w.shape, jnp.float32) for name, w in weights.items()}
    by_weights, _ = lax.scan(take, none_yet, (x, dy))
    gradients = [by_weights[name].astype(jnp.bfloat16).astype(jnp.float32) for name in NAMES]
    gradients = clipped(gradients, sum(jnp.sum(g * g) for g in gradients), sum(g.size for g in gradients))
    new = [
        adamw(w.astype(jnp.float32), m, v, g)
        for w, m, v, g in zip((w_gate, w_up, w_down), (m_w_gate, m_w_up, m_w_down), (v_w_gate, v_w_up, v_w_down), gradients, strict=True)
    ]
    return tuple(one[which] for which in range(3) for one in new)
```

```python
import jax
import jax.numpy as jnp
from jax import lax
from jax.experimental import pallas as pl
from jax.experimental.pallas import tpu as pltpu
from jax.sharding import PartitionSpec as P

D, FF, T = 896, 2560, 4096
IN, OUT = D // 4, FF // 4
CHUNK = 2 * OUT
F32, BF = jnp.float32, jnp.bfloat16
GRANT = 66_000_000
ANY = pl.BlockSpec(memory_space=pl.ANY)


def nn(a, b):
    return lax.dot_general(a, b, (((1,), (0,)), ((), ())), preferred_element_type=F32)


def nt(a, b):
    return lax.dot_general(a, b, (((1,), (1,)), ((), ())), preferred_element_type=F32)


def place(s, me):
    other = s ^ me
    return (other >> 1) | ((other & 1) << 1)


def whole(shape):
    return pl.BlockSpec(shape, lambda *_: (0,) * len(shape), pipeline_mode=pl.Buffered(1))


def rows(bm, width):
    return pl.BlockSpec((bm, width), lambda i, *_: (i, 0))


def cols(height, bm):
    return pl.BlockSpec((height, bm), lambda i, *_: (0, i))


def params():
    return pltpu.CompilerParams(vmem_limit_bytes=GRANT)


def scaled(h):
    wide = h.astype(F32)
    return wide, lax.rsqrt(jnp.mean(wide * wide, -1, keepdims=True) + 1e-6)


def put_rows(me, ref, value):
    for s in range(4):
        at = pl.multiple_of(place(s, me) * IN, 32)
        ref[pl.ds(at, IN), :] = value[s * IN : (s + 1) * IN, :]


def put_columns(me, ref, value, first):
    for k in range(value.shape[1] // OUT):
        at = pl.multiple_of(place(first + k, me) * OUT, 128)
        ref[:, pl.ds(at, OUT)] = value[:, k * OUT : (k + 1) * OUT]


def load_in(layer, me, r, own, got, buf, sem):
    core, x, y, core_x, core_y = got
    at = lambda s: pl.ds(pl.multiple_of(s * IN, 32), IN)
    return [
        pltpu.make_async_copy(own[0].at[layer], buf.at[0, at(me)], sem.at[0]),
        pltpu.make_async_copy(own[1].at[layer], buf.at[1, at(me)], sem.at[1]),
        pltpu.make_async_copy(core, buf.at[:, at(me ^ 1)], sem.at[2]),
        pltpu.make_async_copy(x, buf.at[r, at(me ^ 2)], sem.at[3]),
        pltpu.make_async_copy(y, buf.at[1 - r, at(me ^ 2)], sem.at[4]),
        pltpu.make_async_copy(core_x, buf.at[r, at(me ^ 3)], sem.at[5]),
        pltpu.make_async_copy(core_y, buf.at[1 - r, at(me ^ 3)], sem.at[6]),
    ]


def load_down(layer, r, own, got, buf, sem):
    core, x, y, core_x, core_y = got
    half = OUT // 2
    at = lambda block, which: pl.ds(pl.multiple_of(block * OUT + which * half, 32), half)
    return [
        pltpu.make_async_copy(own.at[layer], buf.at[pl.ds(0, OUT)], sem.at[0]),
        pltpu.make_async_copy(core, buf.at[pl.ds(2 * OUT, OUT)], sem.at[1]),
        pltpu.make_async_copy(x, buf.at[at(1, r)], sem.at[2]),
        pltpu.make_async_copy(y, buf.at[at(1, 1 - r)], sem.at[3]),
        pltpu.make_async_copy(core_x, buf.at[at(3, r)], sem.at[4]),
        pltpu.make_async_copy(core_y, buf.at[at(3, 1 - r)], sem.at[5]),
    ]


SCRATCH = [
    pltpu.VMEM((2, D, FF), BF),
    pltpu.VMEM((FF, D), BF),
    pltpu.SemaphoreType.DMA((7,)),
    pltpu.SemaphoreType.DMA((6,)),
]


def load(where, in_layer, down_layer, refs, scratch):
    own, got_in, got_down = refs[:3], refs[3:8], refs[8:13]
    w_in, w_down, in_sem, down_sem = scratch
    me, r = where[0], where[1]

    @pl.when(pl.program_id(0) == 0)
    def _():
        first = load_in(in_layer, me, r, own, got_in, w_in, in_sem)
        second = load_down(down_layer, r, own[2], got_down, w_down, down_sem)
        for copy in first + second:
            copy.start()
        for copy in first + second:
            copy.wait()


def down_rows(me, w_down, block):
    return w_down[pl.ds(pl.multiple_of(place(block, me) * OUT, OUT), OUT), :]


def first_kernel(where, x_ref, *refs):
    weights, (act_ref, gate_ref, up_ref, h_ref, at_ref), scratch = refs[:13], refs[13:18], refs[18:]
    w_in, w_down = scratch[:2]
    me = where[0]
    load(where, 0, 0, weights, scratch)
    x = x_ref[...]
    wide, scale = scaled(x)
    a = (wide * scale).astype(BF)
    put_rows(me, at_ref, a.T)
    for n in range(0, FF, CHUNK):
        gate = nn(a, w_in[0, :, n : n + CHUNK])
        up = nn(a, w_in[1, :, n : n + CHUNK])
        gate_ref[:, n : n + CHUNK] = gate
        up_ref[:, n : n + CHUNK] = up
        put_columns(me, act_ref, (gate * jax.nn.sigmoid(gate) * up).astype(BF), n // OUT)
    h_ref[...] = x + nn(act_ref[...], w_down[...]).astype(BF)


def first_layer(where, x, weights, bm=512):
    return pl.pallas_call(
        first_kernel,
        grid_spec=pltpu.PrefetchScalarGridSpec(
            num_scalar_prefetch=1,
            grid=(T // bm,),
            in_specs=[rows(bm, D)] + [ANY] * 13,
            out_specs=[rows(bm, FF), rows(bm, FF), rows(bm, FF), rows(bm, D), cols(D, bm)],
            scratch_shapes=SCRATCH,
        ),
        out_shape=[jax.ShapeDtypeStruct((T, FF), dtype) for dtype in (BF, F32, F32)]
        + [jax.ShapeDtypeStruct((T, D), BF), jax.ShapeDtypeStruct((D, T), BF)],
        compiler_params=params(),
        cost_estimate=pl.CostEstimate(flops=6 * T * D * FF, bytes_accessed=140 << 20, transcendentals=0),
        name="first_layer",
    )(where, x, *weights)


def back_through_act(dact, gate, up):
    sig = jax.nn.sigmoid(gate)
    silu = gate * sig
    return silu, (dact * up * (sig * (1.0 + gate - silu))).astype(BF), (dact * silu).astype(BF)


def dact_of(me, dh, w_down, n):
    parts = [nt(dh, down_rows(me, w_down, n // OUT + k)) for k in range(CHUNK // OUT)]
    return jnp.concatenate(parts, axis=1).astype(BF).astype(F32)


def second_kernel(where, h_ref, dy_ref, *refs):
    weights, (act_ref, dgate_ref, dup_ref, at_ref, dyt_ref), scratch = refs[:13], refs[13:18], refs[18:]
    w_in, w_down = scratch[:2]
    me = where[0]
    load(where, 1, 1, weights, scratch)
    wide, scale = scaled(h_ref[...])
    a = (wide * scale).astype(BF)
    put_rows(me, at_ref, a.T)
    dy = dy_ref[...]
    dyt_ref[...] = dy.T
    for n in range(0, FF, CHUNK):
        gate = nn(a, w_in[0, :, n : n + CHUNK])
        up = nn(a, w_in[1, :, n : n + CHUNK])
        silu, dgate, dup = back_through_act(dact_of(me, dy, w_down, n), gate, up)
        put_columns(me, act_ref, (silu * up).astype(BF), n // OUT)
        dgate_ref[:, n : n + CHUNK] = dgate
        dup_ref[:, n : n + CHUNK] = dup


def second_layer(where, h, dy, weights, bm=256):
    return pl.pallas_call(
        second_kernel,
        grid_spec=pltpu.PrefetchScalarGridSpec(
            num_scalar_prefetch=1,
            grid=(T // bm,),
            in_specs=[rows(bm, D), rows(bm, D)] + [ANY] * 13,
            out_specs=[rows(bm, FF)] * 3 + [cols(D, bm)] * 2,
            scratch_shapes=SCRATCH,
        ),
        out_shape=[jax.ShapeDtypeStruct((T, FF), BF)] * 3 + [jax.ShapeDtypeStruct((D, T), BF)] * 2,
        compiler_params=params(),
        cost_estimate=pl.CostEstimate(flops=6 * T * D * FF, bytes_accessed=100 << 20, transcendentals=0),
        name="second_layer",
    )(where, h, dy, *weights)


def between_kernel(where, h_ref, dy_ref, dgate1_ref, dup1_ref, gate_ref, up_ref, *refs):
    weights, (dgate_ref, dup_ref, dht_ref), scratch = refs[:13], refs[13:16], refs[16:]
    w_in, w_down = scratch[:2]
    me = where[0]
    load(where, 1, 0, weights, scratch)
    da = nt(dgate1_ref[...], w_in[0]).astype(BF).astype(F32) + nt(dup1_ref[...], w_in[1]).astype(BF).astype(F32)
    da = da.astype(BF).astype(F32)
    wide, scale = scaled(h_ref[...])
    through = da * scale - wide * (scale * scale * scale * jnp.mean(da * wide, -1, keepdims=True))
    dh = dy_ref[...] + through.astype(BF)
    dht_ref[...] = dh.T
    for n in range(0, FF, CHUNK):
        gate, up = gate_ref[:, n : n + CHUNK], up_ref[:, n : n + CHUNK]
        _, dgate, dup = back_through_act(dact_of(me, dh, w_down, n), gate, up)
        dgate_ref[:, n : n + CHUNK] = dgate
        dup_ref[:, n : n + CHUNK] = dup


def between_layers(where, h, dy, dgate1, dup1, gate, up, weights, bm=256):
    return pl.pallas_call(
        between_kernel,
        grid_spec=pltpu.PrefetchScalarGridSpec(
            num_scalar_prefetch=1,
            grid=(T // bm,),
            in_specs=[rows(bm, D), rows(bm, D)] + [rows(bm, FF)] * 4 + [ANY] * 13,
            out_specs=[rows(bm, FF), rows(bm, FF), cols(D, bm)],
            scratch_shapes=SCRATCH,
        ),
        out_shape=[jax.ShapeDtypeStruct((T, FF), BF)] * 2 + [jax.ShapeDtypeStruct((D, T), BF)],
        compiler_params=params(),
        cost_estimate=pl.CostEstimate(flops=6 * T * D * FF, bytes_accessed=180 << 20, transcendentals=0),
        name="between_layers",
    )(where, h, dy, dgate1, dup1, gate, up, *weights)


def by_in_kernel(left, right, mine_ref, theirs_ref):
    out = nn(left[...], right[...]).astype(BF)
    mine_ref[...] = out[: 2 * IN]
    theirs_ref[...] = out[2 * IN :]


def by_in(at, d, first, width, bn=256):
    tile = pl.BlockSpec((2 * IN, bn), lambda j: (0, j))
    return pl.pallas_call(
        by_in_kernel,
        grid=(width // bn,),
        in_specs=[whole((D, T)), pl.BlockSpec((T, bn), lambda j: (0, j + first // bn))],
        out_specs=[tile, tile],
        out_shape=[jax.ShapeDtypeStruct((2 * IN, width), BF)] * 2,
        compiler_params=params(),
        cost_estimate=pl.CostEstimate(flops=2 * T * D * width, bytes_accessed=40 << 20, transcendentals=0),
        name="by_in",
    )(at, d)


def by_down_kernel(left, right, out_ref):
    out_ref[...] = nn(left[...], right[...]).T.astype(BF)


def by_down(dht, act, first, width, bn=256):
    return pl.pallas_call(
        by_down_kernel,
        grid=(width // bn,),
        in_specs=[whole((D, T)), pl.BlockSpec((T, bn), lambda j: (0, j + first // bn))],
        out_specs=pl.BlockSpec((bn, D), lambda j: (j, 0)),
        out_shape=jax.ShapeDtypeStruct((width, D), BF),
        compiler_params=params(),
        cost_estimate=pl.CostEstimate(flops=2 * T * D * width, bytes_accessed=40 << 20, transcendentals=0),
        name="by_down",
    )(dht, act)


def core(value):
    return lax.ppermute(value, "s", [(i, i ^ 1) for i in range(4)])


def along_x(value):
    return lax.ppermute(value, "s", [(i, i ^ 2) for i in range(4)])


def along_y(value):
    return lax.ppermute(value, "r", [(0, 1), (1, 0)])


def pieces(block, half):
    x = along_x(half)
    y = along_y(x)
    return core(block), x, y, core(x), core(y)


def term(mine, theirs):
    got = core(theirs)
    height = mine.shape[0] // 2
    add = lambda a, b: a.astype(F32) + b.astype(F32)
    x = along_x(add(mine[height:], got[height:]).astype(BF))
    total = (add(mine[:height], got[:height]) + x.astype(F32)).astype(BF)
    return total, along_y(total)


def adamw(w, m, v, g):
    m = 0.9 * m + 0.1 * g
    v = 0.95 * v + 0.05 * g * g
    step = m * lax.rsqrt(v + 1e-8) + 0.1 * w
    return (w - 0.02 * step).astype(jnp.bfloat16), m, v


def clipped(gradients, sum_of_squares, count):
    factor = jnp.minimum(1.0, 0.5 * lax.rsqrt(sum_of_squares / count + 1e-30))
    return [g * factor for g in gradients]


def solution(mesh):
    def step(x, dy, *arrays):
        weights, m, v = (arrays[i : i + 3] for i in (0, 3, 6))
        x, dy = x[0], dy[0]
        me, r = lax.axis_index("s").astype(jnp.int32), lax.axis_index("r").astype(jnp.int32)
        where = jnp.stack([me, r])

        got_in, got_down = [], []
        for layer in range(2):
            both = jnp.stack([weights[0][layer], weights[1][layer]])
            got_in.append(pieces(both, lax.dynamic_index_in_dim(both, r, 0, keepdims=False)))
            block = weights[2][layer]
            got_down.append(pieces(block, lax.dynamic_slice_in_dim(block, r * (OUT // 2), OUT // 2, 0)))
        fetched = lambda i, j: (*weights, *got_in[i], *got_down[j])

        act0, gate0, up0, h, at0 = first_layer(where, x, fetched(0, 0))
        act1, dgate1, dup1, at1, dyt = second_layer(where, h, dy, fetched(1, 1))

        def down(dht, act):
            theirs = by_down(dht, act, 2 * OUT, 2 * OUT)
            return [term(by_down(dht, act, 0, 2 * OUT), theirs)]

        def inner(at, d, parts):
            width = FF // parts
            return [term(*by_in(at, d, i * width, width)) for i in range(parts)]

        down1 = down(dyt, act1)
        gate1, up1 = inner(at1, dgate1, 1), inner(at1, dup1, 1)
        dgate0, dup0, dht = between_layers(where, h, dy, dgate1, dup1, gate0, up0, fetched(1, 0))
        down0 = down(dht, act0)
        gate0, up0 = inner(at0, dgate0, 2), inner(at0, dup0, 2)

        def summed(parts, axis):
            return jnp.concatenate([(a.astype(F32) + b.astype(F32)).astype(BF) for a, b in parts], axis=axis)

        gradients = [
            jnp.stack([summed(first, axis), summed(second, axis)]).astype(F32)
            for first, second, axis in ((gate0, gate1, 1), (up0, up1, 1), (down0, down1, 0))
        ]
        squares = lax.psum(sum(jnp.sum(g * g) for g in gradients), "s")
        gradients = clipped(gradients, squares, lax.psum(1, "s") * sum(g.size for g in gradients))
        new = [adamw(w.astype(F32), m, v, g) for w, m, v, g in zip(weights, m, v, gradients, strict=True)]
        return tuple(one[which] for which in range(3) for one in new)

    states, cut = P(("rep", "r", "s"), None, None), P(None, "s", None)
    return jax.shard_map(
        step,
        mesh=mesh,
        in_specs=(states, states) + (cut,) * 9,
        out_specs=(P("rep", "s", None),) * 9,
        check_vma=False,
    )
```
